32 devices in a mesh: gx: 8 (over z, x), ma: 4 (over y, core).
Axes of the slice: x: 2, y: 2, z: 4, core: 2. Of those that a mesh axis runs over, the one named last changes fastest.
Arguments:
- recorded: float32 [4096, 128, 128], P('ma', 'gx'), may hold values from -51 to 51
- kernel: bfloat16 [2, 8, 4096, 4096], P(None, 'gx', 'ma'), may hold values from -1 to 1
- freq_bins: int32 [8], replicated, may hold values from 1 to 63
- window_start: int32 [4096, 128], P('ma', 'gx'), may hold values from 0 to 31
- window_stop: int32 [4096, 128], P('ma', 'gx'), may hold values from 97 to 128
Outputs:
- solution: float32 [4096, 128, 128], P('ma', 'gx')
- residual: float32 [4096, 128, 128], P('ma', 'gx')
- direction: float32 [4096, 128, 128], P('ma', 'gx')
The draws below stay inside these ranges and needn't reach their ends.
All inputs are finite; a program needn't handle non-finite values.
Results may differ from the reference program's by a relative error of at most 0.015.
Values may be sent and summed in bfloat16 or wider, within the bound.
A program may use at most 128 MiB of HBM per device.

```python
import math
import jax
import jax.numpy as jnp
from jax import lax

NR = 4096
NV = 4096
NT = 128
NS = 128
RAMP = 8
NF = 8


def draw_recorded(key, part):
    key_source = jax.random.fold_in(key, 11)
    key_receiver = jax.random.fold_in(key, 12)
    key_noise = jax.random.fold_in(key, 13)
    key_colour = jax.random.fold_in(key, 15)
    rising = 3.0 ** (jnp.arange(NS, dtype=jnp.float32) / NS)
    source_scale = rising * jnp.exp(jax.random.uniform(key_source, (NS,), jnp.float32) * math.log(10.0))
    receiver_scale = jnp.exp(jax.random.uniform(key_receiver, (NR,), jnp.float32) * math.log(4.0))
    base = jnp.clip(jax.random.normal(key_noise, (NR, NS, NT), jnp.float32), -3.0, 3.0)
    colour = jax.random.uniform(key_colour, (NS,), jnp.float32, -0.9, 0.9)
    delayed = jnp.roll(base, 1, axis=2)
    coloured = (base + colour[None, :, None] * delayed) / jnp.sqrt(1.0 + colour * colour)[None, :, None]
    return 0.1 * coloured * receiver_scale[:, None, None] * source_scale[None, :, None]


def draw_kernel(key, part):
    key_level = jax.random.fold_in(key, 21)
    key_entry = jax.random.fold_in(key, 22)
    level = jnp.exp(jax.random.uniform(key_level, (NF,), jnp.float32, math.log(0.3), math.log(3.0)))
    scale = level[None, :, None, None] / math.sqrt(2.0 * NV)
    entries = jnp.clip(jax.random.normal(key_entry, (2, NF, NR, NV), jnp.float32), -4.0, 4.0)
    return (entries * scale).astype(jnp.bfloat16)


def place_ends(values, own_key, smallest, largest):
    place = [jax.random.randint(jax.random.fold_in(own_key, axis), (), 0, length) for axis, length in enumerate(values.shape)]
    main_axis = values.shape.index(max(values.shape))
    next_to = place[:main_axis] + [(place[main_axis] + 1) % values.shape[main_axis]] + place[main_axis + 1:]
    return values.at[tuple(place)].set(smallest).at[tuple(next_to)].set(largest)


def setup_inputs(seed: int = 0) -> dict:
    keys = jax.random.split(jax.random.key(seed), 6)
    recorded = draw_recorded(jax.random.fold_in(keys[5], 71), 0)
    kernel = draw_kernel(jax.random.fold_in(keys[5], 71), 0)
    freq_bins = place_ends(jax.random.randint(keys[2], (NF,), 1, NT // 2), jax.random.fold_in(keys[2], 1), 1, (NT // 2) - 1).astype(jnp.int32)
    window_start = place_ends(jax.random.randint(keys[3], (NR, NS), 0, NT // 4), jax.random.fold_in(keys[3], 1), 0, (NT // 4) - 1).astype(jnp.int32)
    window_stop = place_ends(jax.random.randint(keys[4], (NR, NS), 3 * NT // 4 + 1, NT + 1), jax.random.fold_in(keys[4], 1), 3 * NT // 4 + 1, NT).astype(jnp.int32)
    return dict(recorded=recorded, kernel=kernel, freq_bins=freq_bins, window_start=window_start, window_stop=window_stop)


epsilon = 1e-06

def phase_table(freq_bins):
    samples = jnp.arange(NT, dtype=jnp.int32)
    angles = (freq_bins[:, None] * samples[None, :] % NT).astype(jnp.float32) * (2.0 * math.pi / NT)
    return jnp.stack([jnp.cos(angles), -jnp.sin(angles)]) * math.sqrt(2.0 / NT)

def taper_weights(window_start, window_stop):
    samples = jnp.arange(NT, dtype=jnp.float32)
    rising = jnp.clip((samples[None, None, :] - window_start[:, :, None].astype(jnp.float32) + 1.0) / RAMP, 0.0, 1.0)
    falling = jnp.clip((window_stop[:, :, None].astype(jnp.float32) - samples[None, None, :]) / RAMP, 0.0, 1.0)
    return rising * falling

def forward_transform(traces, table):
    return jnp.einsum('ast,cft->facs', traces, table, precision=lax.Precision.HIGHEST).astype(jnp.bfloat16)

def inverse_transform(spectra, table):
    return jnp.einsum('facs,cft->ast', spectra.astype(jnp.float32), table, precision=lax.Precision.HIGHEST)

def forward_apply(model_traces, kernel, table, weights):
    spectra = forward_transform(model_traces, table)

    def per_freq(index):
        gains = lax.dynamic_index_in_dim(kernel, index, 1, keepdims=False)
        incoming = lax.dynamic_index_in_dim(spectra, index, 0, keepdims=False)
        real_in = incoming[:, 0, :]
        imag_in = incoming[:, 1, :]
        real_out = jnp.dot(gains[0], real_in, preferred_element_type=jnp.float32) - jnp.dot(gains[1], imag_in, preferred_element_type=jnp.float32)
        imag_out = jnp.dot(gains[0], imag_in, preferred_element_type=jnp.float32) + jnp.dot(gains[1], real_in, preferred_element_type=jnp.float32)
        return jnp.stack([real_out, imag_out], 1).astype(jnp.bfloat16)
    result = lax.map(per_freq, jnp.arange(NF, dtype=jnp.int32))
    return weights * inverse_transform(result, table)

def adjoint_apply(data_traces, kernel, table, weights):
    spectra = forward_transform(weights * data_traces, table)

    def per_freq(index):
        gains = lax.dynamic_index_in_dim(kernel, index, 1, keepdims=False)
        incoming = lax.dynamic_index_in_dim(spectra, index, 0, keepdims=False)
        real_in = incoming[:, 0, :]
        imag_in = incoming[:, 1, :]
        real_out = jnp.dot(gains[0].T, real_in, preferred_element_type=jnp.float32) + jnp.dot(gains[1].T, imag_in, preferred_element_type=jnp.float32)
        imag_out = jnp.dot(gains[0].T, imag_in, preferred_element_type=jnp.float32) - jnp.dot(gains[1].T, real_in, preferred_element_type=jnp.float32)
        return jnp.stack([real_out, imag_out], 1).astype(jnp.bfloat16)
    result = lax.map(per_freq, jnp.arange(NF, dtype=jnp.int32))
    return inverse_transform(result, table)

def reference(recorded, kernel, freq_bins, window_start, window_stop):
    table = phase_table(freq_bins)
    weights = taper_weights(window_start, window_stop)
    gradient = adjoint_apply(recorded, kernel, table, weights)
    norm_start = jnp.sum(gradient * gradient)
    data_image = forward_apply(gradient, kernel, table, weights)
    norm_data = jnp.sum(data_image * data_image)
    step_size = norm_start / (norm_data + epsilon)
    solution = step_size * gradient
    residual = recorded - step_size * data_image
    gradient_new = adjoint_apply(residual, kernel, table, weights)
    norm_final = jnp.sum(gradient_new * gradient_new)
    direction = gradient_new + norm_final / (norm_start + epsilon) * gradient
    return (solution, residual, direction)
```

```python
import functools
import math

import jax
import jax.numpy as jnp
from jax import lax
from jax.experimental import pallas as pl
from jax.experimental.pallas import tpu as pltpu
from jax.sharding import PartitionSpec as P

RAMP = 8
MESH = pl.DeviceIdType.MESH

epsilon = 1e-06


def phase_table(freq_bins, length):
    samples = jnp.arange(length, dtype=jnp.int32)
    angles = (freq_bins[:, None] * samples[None, :] % length).astype(jnp.float32) * (
        2.0 * math.pi / length
    )
    return jnp.stack([jnp.cos(angles), -jnp.sin(angles)], 1) * math.sqrt(2.0 / length)


def taper_weights(window_start, window_stop, length):
    samples = jnp.arange(length, dtype=jnp.float32)
    rising = jnp.clip(
        (samples[None, None, :] - window_start[:, :, None].astype(jnp.float32) + 1.0) / RAMP,
        0.0,
        1.0,
    )
    falling = jnp.clip(
        (window_stop[:, :, None].astype(jnp.float32) - samples[None, None, :]) / RAMP, 0.0, 1.0
    )
    return rising * falling


def exchange_kernel(n, x_ref, o_ref, send_sem, recv_sem, own_sem):
    me = lax.axis_index("gx")
    barrier = pltpu.get_barrier_semaphore()
    for k in range(1, n):
        pl.semaphore_signal(
            barrier, inc=1, device_id={"gx": lax.rem(me + k, n)}, device_id_type=MESH
        )
    own = pltpu.make_async_copy(x_ref.at[me], o_ref.at[me], own_sem)
    own.start()
    pl.semaphore_wait(barrier, n - 1)
    copies = []
    for k in range(1, n):
        peer = lax.rem(me + k, n)
        copy = pltpu.make_async_remote_copy(
            src_ref=x_ref.at[peer],
            dst_ref=o_ref.at[me],
            send_sem=send_sem.at[k],
            recv_sem=recv_sem.at[k],
            device_id={"gx": peer},
            device_id_type=MESH,
        )
        copy.start()
        copies.append(copy)
    own.wait()
    for copy in copies:
        copy.wait()


def exchange(x, n, number):
    return pl.pallas_call(
        functools.partial(exchange_kernel, n),
        out_shape=jax.ShapeDtypeStruct(x.shape, x.dtype),
        in_specs=[pl.BlockSpec(memory_space=pltpu.VMEM)],
        out_specs=pl.BlockSpec(memory_space=pltpu.VMEM),
        scratch_shapes=[
            pltpu.SemaphoreType.DMA((n,)),
            pltpu.SemaphoreType.DMA((n,)),
            pltpu.SemaphoreType.DMA,
        ],
        compiler_params=pltpu.CompilerParams(collective_id=number, has_side_effects=True),
        name=f"exchange{number}",
    )(x)


def total_kernel(outer, inner, x_ref, o_ref, held, send_sem, recv_sem):
    n = outer * inner
    me = lax.axis_index("gx") * inner + lax.axis_index("ma")
    barrier = pltpu.get_barrier_semaphore()

    def place(k):
        peer = lax.rem(me + k, n)
        return (peer // inner, lax.rem(peer, inner))

    for k in range(1, n):
        pl.semaphore_signal(barrier, inc=1, device_id=place(k), device_id_type=MESH)
    pl.semaphore_wait(barrier, n - 1)
    copies = []
    for k in range(1, n):
        copy = pltpu.make_async_remote_copy(
            src_ref=x_ref,
            dst_ref=held.at[me],
            send_sem=send_sem.at[k],
            recv_sem=recv_sem.at[k],
            device_id=place(k),
            device_id_type=MESH,
        )
        copy.start()
        copies.append(copy)
    held[me] = x_ref[...]
    for copy in copies:
        copy.wait()
    o_ref[...] = jnp.sum(held[...], axis=0)


def total(x, outer, inner, number):
    n = outer * inner
    return pl.pallas_call(
        functools.partial(total_kernel, outer, inner),
        out_shape=jax.ShapeDtypeStruct(x.shape, x.dtype),
        in_specs=[pl.BlockSpec(memory_space=pltpu.VMEM)],
        out_specs=pl.BlockSpec(memory_space=pltpu.VMEM),
        scratch_shapes=[
            pltpu.VMEM((n,) + x.shape, x.dtype),
            pltpu.SemaphoreType.DMA((n,)),
            pltpu.SemaphoreType.DMA((n,)),
        ],
        compiler_params=pltpu.CompilerParams(collective_id=number, has_side_effects=True),
        name=f"total{number}",
    )(x)


def pairs(n, bit):
    return [(i, i ^ bit) for i in range(n)]


def scatter_sum(partial, n):
    rows, block = partial.shape[1:]
    me = lax.axis_index("ma")
    held = partial
    bit = 1
    while bit < n:
        own = (me // bit) % 2
        parts = held.reshape(-1, 2, rows, block)
        keep = lax.dynamic_index_in_dim(parts, own, 1, keepdims=False)
        send = lax.dynamic_index_in_dim(parts, 1 - own, 1, keepdims=False)
        got = lax.ppermute(send, "ma", pairs(n, bit))
        held = (keep.astype(jnp.float32) + got.astype(jnp.float32)).astype(jnp.bfloat16)
        bit *= 2
    return held.reshape(rows, block)


def gather_all(x, n):
    rows, block = x.shape
    me = lax.axis_index("ma")
    held = x.reshape(rows, 1, block)
    bit = n // 2
    while bit >= 1:
        own = (me // bit) % 2
        got = lax.ppermute(held, "ma", pairs(n, bit))
        first = jnp.where(own == 0, held, got)
        second = jnp.where(own == 0, got, held)
        held = jnp.stack([first, second], 2).reshape(rows, -1, block)
        bit //= 2
    return held.reshape(rows, n * block)


def to_spectra(traces, table):
    freqs = table.shape[0]
    flat = table.reshape(2 * freqs, table.shape[2]).astype(jnp.bfloat16)
    out = jnp.einsum(
        "ast,kt->ksa", traces.astype(jnp.bfloat16), flat, preferred_element_type=jnp.float32
    ).astype(jnp.bfloat16)
    return out.reshape(freqs, 2 * out.shape[1], out.shape[2])


def to_traces(spectra, table):
    freqs, double, points = spectra.shape
    sources = double // 2
    length = table.shape[2]
    depth = freqs * double
    across = spectra.reshape(depth, points).T
    owner = jnp.arange(depth, dtype=jnp.int32) % sources
    mask = (owner[None, :] == jnp.arange(sources, dtype=jnp.int32)[:, None]).astype(jnp.bfloat16)
    spread = (across[:, None, :] * mask[None]).reshape(points * sources, depth)
    tall = jnp.repeat(table.reshape(2 * freqs, length).astype(jnp.bfloat16), sources, axis=0)
    out = jnp.dot(spread, tall, preferred_element_type=jnp.float32)
    return out.reshape(points, sources, length)


def by_frequency(arrived, n):
    sources = arrived.shape[1] // 2
    points = arrived.shape[2]
    return arrived.reshape(n, 2, sources, points).transpose(1, 0, 2, 3).reshape(2, -1, points)


def by_source(spectra, n):
    points = spectra.shape[2]
    sources = spectra.shape[1] // n
    return spectra.reshape(2, n, sources, points).transpose(1, 0, 2, 3).reshape(n, -1, points)


def adjoint_kernel(d_ref, k_ref, o_ref):
    half = d_ref.shape[0] // 2
    data = d_ref[...]
    first = jnp.dot(data, k_ref[0], preferred_element_type=jnp.float32)
    second = jnp.dot(data, k_ref[1], preferred_element_type=jnp.float32)
    o_ref[0, :half] = (first[:half] + second[half:]).astype(o_ref.dtype)
    o_ref[0, half:] = (first[half:] - second[:half]).astype(o_ref.dtype)


def adjoint_product(data, flat_kernel, inner):
    sources, rows = data.shape[1], data.shape[2]
    columns = flat_kernel.shape[1]
    block = columns // inner
    tile = min(512, block)
    per_block = block // tile
    partial = pl.pallas_call(
        adjoint_kernel,
        grid=(columns // tile,),
        out_shape=jax.ShapeDtypeStruct((inner, 2 * sources, block), jnp.bfloat16),
        in_specs=[
            pl.BlockSpec((2 * sources, rows), lambda j: (0, 0)),
            pl.BlockSpec((2, rows, tile), lambda j: (0, 0, j)),
        ],
        out_specs=pl.BlockSpec(
            (1, 2 * sources, tile), lambda j: (j // per_block, 0, j % per_block)
        ),
        compiler_params=pltpu.CompilerParams(vmem_limit_bytes=60 * 1024 * 1024),
        cost_estimate=pl.CostEstimate(
            flops=8 * sources * rows * columns,
            bytes_accessed=4 * rows * columns + 4 * sources * (rows + columns),
            transcendentals=0,
        ),
        name="adjoint",
    )(data.reshape(2 * sources, rows), flat_kernel.reshape(2, rows, columns))
    return scatter_sum(partial, inner).reshape(2, sources, block)


def final_kernel(
    sums_ref, rec_ref, win_ref, g_ref, d_ref, h_ref, tall_ref, mask_ref, pick_ref,
    sol_ref, res_ref, dir_ref,
):
    tile, sources, length = rec_ref.shape
    norm_start, norm_data = sums_ref[0, 0], sums_ref[1, 0]
    cross, norm_change = sums_ref[2, 0], sums_ref[3, 0]
    step_size = norm_start / (norm_data + epsilon)
    norm_final = norm_start - 2.0 * step_size * cross + step_size * step_size * norm_change
    ratio = norm_final / (norm_start + epsilon)
    tall = tall_ref[...]

    def rows(values, mask):
        return (values[:, None, :] * mask[None]).reshape(tile * sources, -1).astype(jnp.bfloat16)

    def traces(ref):
        spread = rows(ref[...].astype(jnp.float32), mask_ref[...])
        out = jnp.dot(spread, tall, preferred_element_type=jnp.float32)
        return out.reshape(tile, sources, length)

    gradient = traces(g_ref)
    change = traces(h_ref)
    sol_ref[...] = step_size * gradient
    dir_ref[...] = (gradient - step_size * change) + ratio * gradient
    window = win_ref[...]
    ones = jnp.ones((window.shape[1], length), jnp.bfloat16)
    shape = (tile, sources, length)
    start = jnp.dot(rows(window, pick_ref[0]), ones, preferred_element_type=jnp.float32)
    stop = jnp.dot(rows(window, pick_ref[1]), ones, preferred_element_type=jnp.float32)
    samples = lax.broadcasted_iota(jnp.int32, shape, 2).astype(jnp.float32)
    rising = jnp.clip((samples - start.reshape(shape) + 1.0) / RAMP, 0.0, 1.0)
    falling = jnp.clip((stop.reshape(shape) - samples) / RAMP, 0.0, 1.0)
    image = (rising * falling) * traces(d_ref)
    res_ref[...] = rec_ref[...] - step_size * image


def final_step(sums, recorded, window_start, window_stop, returned, arrived, changed, table):
    points, sources, length = recorded.shape
    depth = returned.shape[0] * returned.shape[1]
    tile = min(128, points)

    def across(x):
        return x.reshape(depth, points).T

    place = jnp.arange(sources, dtype=jnp.int32)
    owner = jnp.arange(depth, dtype=jnp.int32) % sources
    mask = (owner[None, :] == place[:, None]).astype(jnp.float32)
    column = jnp.arange(2 * sources, dtype=jnp.int32)
    pick = jnp.stack(
        [column[None, :] == place[:, None], column[None, :] == place[:, None] + sources]
    ).astype(jnp.float32)
    tall = jnp.repeat(table.reshape(-1, length).astype(jnp.bfloat16), sources, axis=0)
    window = jnp.concatenate([window_start, window_stop], 1).astype(jnp.float32)
    whole3 = pl.BlockSpec((tile, sources, length), lambda i: (i, 0, 0))
    strip = pl.BlockSpec((tile, depth), lambda i: (i, 0))
    return pl.pallas_call(
        final_kernel,
        grid=(points // tile,),
        out_shape=[jax.ShapeDtypeStruct(recorded.shape, jnp.float32)] * 3,
        in_specs=[
            pl.BlockSpec(memory_space=pltpu.SMEM),
            whole3,
            pl.BlockSpec((tile, 2 * sources), lambda i: (i, 0)),
            strip,
            strip,
            strip,
            pl.BlockSpec((depth, length), lambda i: (0, 0)),
            pl.BlockSpec((sources, depth), lambda i: (0, 0)),
            pl.BlockSpec((2, sources, 2 * sources), lambda i: (0, 0, 0)),
        ],
        out_specs=[whole3] * 3,
        compiler_params=pltpu.CompilerParams(vmem_limit_bytes=48 * 1024 * 1024),
        cost_estimate=pl.CostEstimate(
            flops=8 * points * sources * depth * length,
            bytes_accessed=16 * points * sources * length,
            transcendentals=0,
        ),
        name="final",
    )(sums, recorded, window, across(returned), across(arrived), across(changed), tall, mask, pick)


def forward_product(model, flat_kernel, inner):
    sources = model.shape[1]
    incoming = gather_all(model.reshape(2 * sources, -1), inner)
    product = lax.dot_general(
        incoming, flat_kernel, (((1,), (1,)), ((), ())), preferred_element_type=jnp.float32
    )
    half = flat_kernel.shape[0] // 2
    real_part = product[:sources, :half] - product[sources:, half:]
    imaginary = product[sources:, :half] + product[:sources, half:]
    return jnp.stack([real_part, imaginary], 0).astype(jnp.bfloat16)


def per_device(outer, inner, recorded, kernel, freq_bins, window_start, window_stop):
    length = recorded.shape[2]
    table = phase_table(freq_bins, length)
    weights = taper_weights(window_start, window_stop, length)
    flat_kernel = kernel.reshape(2 * kernel.shape[2], kernel.shape[3])

    data = by_frequency(exchange(to_spectra(weights * recorded, table), outer, 0), outer)
    adjoint = adjoint_product(data, flat_kernel, inner)
    returned = lax.all_to_all(
        by_source(adjoint, outer), "gx", split_axis=0, concat_axis=0, tiled=True
    )

    same = freq_bins[:, None] == freq_bins[None, :]
    repeated = jnp.sum(same.astype(jnp.int32)) > freq_bins.shape[0]

    def combined(spectra):
        parts = lax.all_to_all(
            by_source(spectra, outer), "gx", split_axis=0, concat_axis=0, tiled=True
        )
        mixed = jnp.einsum(
            "gf,fxa->gxa",
            same.astype(jnp.bfloat16),
            parts,
            preferred_element_type=jnp.float32,
        ).astype(jnp.bfloat16)
        back = lax.all_to_all(mixed, "gx", split_axis=0, concat_axis=0, tiled=True)
        return by_frequency(back, outer)

    model = lax.cond(repeated, combined, lambda spectra: spectra, adjoint)
    outgoing = by_source(forward_product(model, flat_kernel, inner), outer)
    imaged = exchange(outgoing, outer, 1)
    image = weights * to_traces(imaged, table)
    second = by_frequency(exchange(to_spectra(weights * image, table), outer, 2), outer)
    normal = adjoint_product(second, flat_kernel, inner)
    changed = exchange(by_source(normal, outer), outer, 3)

    double, points = returned.shape[1:]
    depth = freq_bins.shape[0] * double
    eye = jnp.eye(double, dtype=jnp.bfloat16)
    mixing = (same.astype(jnp.bfloat16)[:, None, :, None] * eye[None, :, None, :]).reshape(
        depth, depth
    )
    flat_g = returned.reshape(depth, points)
    flat_h = changed.reshape(depth, points)
    mixed_g = jnp.dot(mixing, flat_g, preferred_element_type=jnp.float32)
    mixed_h = jnp.dot(mixing, flat_h, preferred_element_type=jnp.float32)
    sums = jnp.stack(
        [
            jnp.sum(flat_g.astype(jnp.float32) * mixed_g),
            jnp.sum(image * image),
            jnp.sum(mixed_g * flat_h.astype(jnp.float32)),
            jnp.sum(flat_h.astype(jnp.float32) * mixed_h),
        ]
    )
    sums = total(jnp.broadcast_to(jnp.tile(sums, 2)[:, None], (8, 128)), outer, inner, 4)
    if recorded.shape[1] % 8 == 0:
        return tuple(
            final_step(
                sums, recorded, window_start, window_stop, returned, imaged, changed, table
            )
        )
    gradient = to_traces(returned, table)
    change = to_traces(changed, table)
    norm_start, norm_data, cross, norm_change = sums[0, 0], sums[1, 0], sums[2, 0], sums[3, 0]
    step_size = norm_start / (norm_data + epsilon)
    norm_final = norm_start - 2.0 * step_size * cross + step_size * step_size * norm_change
    solution = step_size * gradient
    residual = recorded - step_size * image
    direction = gradient - step_size * change + norm_final / (norm_start + epsilon) * gradient
    return (solution, residual, direction)


def solution(mesh):
    in_specs = (P("ma", "gx", None), P(None, "gx", "ma", None), P(), P("ma", "gx"), P("ma", "gx"))
    out_specs = (P("ma", "gx", None), P("ma", "gx", None), P("ma", "gx", None))
    return jax.shard_map(
        functools.partial(per_device, mesh.shape["gx"], mesh.shape["ma"]),
        mesh=mesh,
        in_specs=in_specs,
        out_specs=out_specs,
        check_vma=False,
    )
```

```python
import functools
import math

import jax
import jax.numpy as jnp
from jax import lax
from jax.experimental import pallas as pl
from jax.experimental.pallas import tpu as pltpu
from jax.sharding import PartitionSpec as P

RAMP = 8
MESH = pl.DeviceIdType.MESH

epsilon = 1e-06


def phase_table(freq_bins, length):
    samples = jnp.arange(length, dtype=jnp.int32)
    angles = (freq_bins[:, None] * samples[None, :] % length).astype(jnp.float32) * (
        2.0 * math.pi / length
    )
    return jnp.stack([jnp.cos(angles), -jnp.sin(angles)], 1) * math.sqrt(2.0 / length)


def taper_weights(window_start, window_stop, length):
    samples = jnp.arange(length, dtype=jnp.float32)
    rising = jnp.clip(
        (samples[None, None, :] - window_start[:, :, None].astype(jnp.float32) + 1.0) / RAMP,
        0.0,
        1.0,
    )
    falling = jnp.clip(
        (window_stop[:, :, None].astype(jnp.float32) - samples[None, None, :]) / RAMP, 0.0, 1.0
    )
    return rising * falling


def exchange_kernel(n, x_ref, o_ref, send_sem, recv_sem, own_sem):
    me = lax.axis_index("gx")
    barrier = pltpu.get_barrier_semaphore()
    for k in range(1, n):
        pl.semaphore_signal(
            barrier, inc=1, device_id={"gx": lax.rem(me + k, n)}, device_id_type=MESH
        )
    own = pltpu.make_async_copy(x_ref.at[me], o_ref.at[me], own_sem)
    own.start()
    pl.semaphore_wait(barrier, n - 1)
    copies = []
    for k in range(1, n):
        peer = lax.rem(me + k, n)
        copy = pltpu.make_async_remote_copy(
            src_ref=x_ref.at[peer],
            dst_ref=o_ref.at[me],
            send_sem=send_sem.at[k],
            recv_sem=recv_sem.at[k],
            device_id={"gx": peer},
            device_id_type=MESH,
        )
        copy.start()
        copies.append(copy)
    own.wait()
    for copy in copies:
        copy.wait()


def exchange(x, n, number):
    return pl.pallas_call(
        functools.partial(exchange_kernel, n),
        out_shape=jax.ShapeDtypeStruct(x.shape, x.dtype),
        in_specs=[pl.BlockSpec(memory_space=pltpu.VMEM)],
        out_specs=pl.BlockSpec(memory_space=pltpu.VMEM),
        scratch_shapes=[
            pltpu.SemaphoreType.DMA((n,)),
            pltpu.SemaphoreType.DMA((n,)),
            pltpu.SemaphoreType.DMA,
        ],
        compiler_params=pltpu.CompilerParams(collective_id=number, has_side_effects=True),
        name=f"exchange{number}",
    )(x)


def total_kernel(n, axis, x_ref, o_ref, held, send_sem, recv_sem):
    me = lax.axis_index(axis)
    barrier = pltpu.get_barrier_semaphore()
    for k in range(1, n):
        pl.semaphore_signal(
            barrier, inc=1, device_id={axis: lax.rem(me + k, n)}, device_id_type=MESH
        )
    pl.semaphore_wait(barrier, n - 1)
    copies = []
    for k in range(1, n):
        copy = pltpu.make_async_remote_copy(
            src_ref=x_ref,
            dst_ref=held.at[me],
            send_sem=send_sem.at[k],
            recv_sem=recv_sem.at[k],
            device_id={axis: lax.rem(me + k, n)},
            device_id_type=MESH,
        )
        copy.start()
        copies.append(copy)
    held[me] = x_ref[...]
    for copy in copies:
        copy.wait()
    o_ref[...] = jnp.sum(held[...], axis=0)


def total(x, n, axis, number):
    return pl.pallas_call(
        functools.partial(total_kernel, n, axis),
        out_shape=jax.ShapeDtypeStruct(x.shape, x.dtype),
        in_specs=[pl.BlockSpec(memory_space=pltpu.VMEM)],
        out_specs=pl.BlockSpec(memory_space=pltpu.VMEM),
        scratch_shapes=[
            pltpu.VMEM((n,) + x.shape, x.dtype),
            pltpu.SemaphoreType.DMA((n,)),
            pltpu.SemaphoreType.DMA((n,)),
        ],
        compiler_params=pltpu.CompilerParams(collective_id=number, has_side_effects=True),
        name=f"total{number}",
    )(x)


def pairs(n, bit):
    return [(i, i ^ bit) for i in range(n)]


def scatter_sum(partial, n):
    rows, block = partial.shape[1:]
    me = lax.axis_index("ma")
    held = partial
    bit = 1
    while bit < n:
        own = (me // bit) % 2
        parts = held.reshape(-1, 2, rows, block)
        keep = lax.dynamic_index_in_dim(parts, own, 1, keepdims=False)
        send = lax.dynamic_index_in_dim(parts, 1 - own, 1, keepdims=False)
        got = lax.ppermute(send, "ma", pairs(n, bit))
        held = (keep.astype(jnp.float32) + got.astype(jnp.float32)).astype(jnp.bfloat16)
        bit *= 2
    return held.reshape(rows, block)


def gather_all(x, n):
    rows, block = x.shape
    me = lax.axis_index("ma")
    held = x[None]
    bit = n // 2
    while bit >= 1:
        own = (me // bit) % 2
        got = lax.ppermute(held, "ma", pairs(n, bit))
        first = jnp.where(own == 0, held, got)
        second = jnp.where(own == 0, got, held)
        held = jnp.stack([first, second], 1).reshape(-1, rows, block)
        bit //= 2
    return held


def to_spectra(traces, table):
    freqs = table.shape[0]
    flat = table.reshape(2 * freqs, table.shape[2]).astype(jnp.bfloat16)
    out = jnp.einsum(
        "ast,kt->ksa", traces.astype(jnp.bfloat16), flat, preferred_element_type=jnp.float32
    ).astype(jnp.bfloat16)
    return out.reshape(freqs, 2 * out.shape[1], out.shape[2])


def to_traces(spectra, table):
    freqs, double, points = spectra.shape
    sources = double // 2
    length = table.shape[2]
    depth = freqs * double
    across = spectra.reshape(depth, points).T
    owner = jnp.arange(depth, dtype=jnp.int32) % sources
    mask = (owner[None, :] == jnp.arange(sources, dtype=jnp.int32)[:, None]).astype(jnp.bfloat16)
    spread = (across[:, None, :] * mask[None]).reshape(points * sources, depth)
    tall = jnp.repeat(table.reshape(2 * freqs, length).astype(jnp.bfloat16), sources, axis=0)
    out = jnp.dot(spread, tall, preferred_element_type=jnp.float32)
    return out.reshape(points, sources, length)


def by_frequency(arrived, n):
    sources = arrived.shape[1] // 2
    points = arrived.shape[2]
    return arrived.reshape(n, 2, sources, points).transpose(1, 0, 2, 3).reshape(2, -1, points)


def by_source(spectra, n):
    points = spectra.shape[2]
    sources = spectra.shape[1] // n
    return spectra.reshape(2, n, sources, points).transpose(1, 0, 2, 3).reshape(n, -1, points)


def adjoint_kernel(d_ref, k_ref, o_ref):
    half = d_ref.shape[0] // 2
    data = d_ref[...]
    first = jnp.dot(data, k_ref[0], preferred_element_type=jnp.float32)
    second = jnp.dot(data, k_ref[1], preferred_element_type=jnp.float32)
    o_ref[0, :half] = (first[:half] + second[half:]).astype(o_ref.dtype)
    o_ref[0, half:] = (first[half:] - second[:half]).astype(o_ref.dtype)


def adjoint_product(data, flat_kernel, inner):
    sources, rows = data.shape[1], data.shape[2]
    columns = flat_kernel.shape[1]
    block = columns // inner
    tile = min(512, block)
    per_block = block // tile
    partial = pl.pallas_call(
        adjoint_kernel,
        grid=(columns // tile,),
        out_shape=jax.ShapeDtypeStruct((inner, 2 * sources, block), jnp.bfloat16),
        in_specs=[
            pl.BlockSpec((2 * sources, rows), lambda j: (0, 0)),
            pl.BlockSpec((2, rows, tile), lambda j: (0, 0, j)),
        ],
        out_specs=pl.BlockSpec(
            (1, 2 * sources, tile), lambda j: (j // per_block, 0, j % per_block)
        ),
        compiler_params=pltpu.CompilerParams(vmem_limit_bytes=60 * 1024 * 1024),
        cost_estimate=pl.CostEstimate(
            flops=8 * sources * rows * columns,
            bytes_accessed=4 * rows * columns + 4 * sources * (rows + columns),
            transcendentals=0,
        ),
        name="adjoint",
    )(data.reshape(2 * sources, rows), flat_kernel.reshape(2, rows, columns))
    return scatter_sum(partial, inner).reshape(2, sources, block)


def final_kernel(
    sums_ref, rec_ref, win_ref, g_ref, d_ref, h_ref, tall_ref, mask_ref, pick_ref,
    sol_ref, res_ref, dir_ref,
):
    tile, sources, length = rec_ref.shape
    norm_start, norm_data = sums_ref[0, 0], sums_ref[1, 0]
    cross, norm_change = sums_ref[2, 0], sums_ref[3, 0]
    step_size = norm_start / (norm_data + epsilon)
    norm_final = norm_start - 2.0 * step_size * cross + step_size * step_size * norm_change
    ratio = norm_final / (norm_start + epsilon)
    tall = tall_ref[...]

    def rows(values, mask):
        return (values[:, None, :] * mask[None]).reshape(tile * sources, -1).astype(jnp.bfloat16)

    def traces(ref):
        spread = rows(ref[...].astype(jnp.float32), mask_ref[...])
        out = jnp.dot(spread, tall, preferred_element_type=jnp.float32)
        return out.reshape(tile, sources, length)

    gradient = traces(g_ref)
    change = traces(h_ref)
    sol_ref[...] = step_size * gradient
    dir_ref[...] = (gradient - step_size * change) + ratio * gradient
    window = win_ref[...]
    ones = jnp.ones((window.shape[1], length), jnp.bfloat16)
    shape = (tile, sources, length)
    start = jnp.dot(rows(window, pick_ref[0]), ones, preferred_element_type=jnp.float32)
    stop = jnp.dot(rows(window, pick_ref[1]), ones, preferred_element_type=jnp.float32)
    samples = lax.broadcasted_iota(jnp.int32, shape, 2).astype(jnp.float32)
    rising = jnp.clip((samples - start.reshape(shape) + 1.0) / RAMP, 0.0, 1.0)
    falling = jnp.clip((stop.reshape(shape) - samples) / RAMP, 0.0, 1.0)
    image = (rising * falling) * traces(d_ref)
    res_ref[...] = rec_ref[...] - step_size * image


def final_step(sums, recorded, window_start, window_stop, returned, arrived, changed, table):
    points, sources, length = recorded.shape
    depth = returned.shape[0] * returned.shape[1]
    tile = min(128, points)

    def across(x):
        return x.reshape(depth, points).T

    place = jnp.arange(sources, dtype=jnp.int32)
    owner = jnp.arange(depth, dtype=jnp.int32) % sources
    mask = (owner[None, :] == place[:, None]).astype(jnp.float32)
    column = jnp.arange(2 * sources, dtype=jnp.int32)
    pick = jnp.stack(
        [column[None, :] == place[:, None], column[None, :] == place[:, None] + sources]
    ).astype(jnp.float32)
    tall = jnp.repeat(table.reshape(-1, length).astype(jnp.bfloat16), sources, axis=0)
    window = jnp.concatenate([window_start, window_stop], 1).astype(jnp.float32)
    whole3 = pl.BlockSpec((tile, sources, length), lambda i: (i, 0, 0))
    strip = pl.BlockSpec((tile, depth), lambda i: (i, 0))
    return pl.pallas_call(
        final_kernel,
        grid=(points // tile,),
        out_shape=[jax.ShapeDtypeStruct(recorded.shape, jnp.float32)] * 3,
        in_specs=[
            pl.BlockSpec(memory_space=pltpu.SMEM),
            whole3,
            pl.BlockSpec((tile, 2 * sources), lambda i: (i, 0)),
            strip,
            strip,
            strip,
            pl.BlockSpec((depth, length), lambda i: (0, 0)),
            pl.BlockSpec((sources, depth), lambda i: (0, 0)),
            pl.BlockSpec((2, sources, 2 * sources), lambda i: (0, 0, 0)),
        ],
        out_specs=[whole3] * 3,
        compiler_params=pltpu.CompilerParams(vmem_limit_bytes=48 * 1024 * 1024),
        cost_estimate=pl.CostEstimate(
            flops=8 * points * sources * depth * length,
            bytes_accessed=16 * points * sources * length,
            transcendentals=0,
        ),
        name="final",
    )(sums, recorded, window, across(returned), across(arrived), across(changed), tall, mask, pick)


def forward_kernel(n, x_ref, k_ref, o_ref):
    half = x_ref.shape[1] // 2
    block = x_ref.shape[2]
    totals = []
    for part in range(2):
        total_part = None
        for i in range(n):
            term = lax.dot_general(
                x_ref[i],
                k_ref[part, :, i * block : (i + 1) * block],
                (((1,), (1,)), ((), ())),
                preferred_element_type=jnp.float32,
            )
            total_part = term if total_part is None else total_part + term
        totals.append(total_part)
    first, second = totals
    o_ref[:half] = (first[:half] - second[half:]).astype(o_ref.dtype)
    o_ref[half:] = (first[half:] + second[:half]).astype(o_ref.dtype)


def forward_product(model, flat_kernel, inner):
    sources = model.shape[1]
    incoming = gather_all(model.reshape(2 * sources, -1), inner)
    rows, columns = flat_kernel.shape[0] // 2, flat_kernel.shape[1]
    tile = min(256, rows)
    product = pl.pallas_call(
        functools.partial(forward_kernel, inner),
        grid=(rows // tile,),
        out_shape=jax.ShapeDtypeStruct((2 * sources, rows), jnp.bfloat16),
        in_specs=[
            pl.BlockSpec(incoming.shape, lambda j: (0, 0, 0)),
            pl.BlockSpec((2, tile, columns), lambda j: (0, j, 0)),
        ],
        out_specs=pl.BlockSpec((2 * sources, tile), lambda j: (0, j)),
        compiler_params=pltpu.CompilerParams(vmem_limit_bytes=60 * 1024 * 1024),
        cost_estimate=pl.CostEstimate(
            flops=8 * sources * rows * columns,
            bytes_accessed=4 * rows * columns + 4 * sources * (rows + columns),
            transcendentals=0,
        ),
        name="forward",
    )(incoming, flat_kernel.reshape(2, rows, columns))
    return product.reshape(2, sources, rows)


def per_device(outer, inner, recorded, kernel, freq_bins, window_start, window_stop):
    length = recorded.shape[2]
    table = phase_table(freq_bins, length)
    weights = taper_weights(window_start, window_stop, length)
    flat_kernel = kernel.reshape(2 * kernel.shape[2], kernel.shape[3])

    data = by_frequency(exchange(to_spectra(weights * recorded, table), outer, 0), outer)
    adjoint = adjoint_product(data, flat_kernel, inner)
    returned = exchange(by_source(adjoint, outer), outer, 6)

    same = freq_bins[:, None] == freq_bins[None, :]
    repeated = jnp.sum(same.astype(jnp.int32)) > freq_bins.shape[0]

    def combined(spectra, parts):
        mixed = jnp.einsum(
            "gf,fxa->gxa",
            same.astype(jnp.bfloat16),
            parts,
            preferred_element_type=jnp.float32,
        ).astype(jnp.bfloat16)
        return by_frequency(exchange(mixed, outer, 7), outer)

    model = lax.cond(repeated, combined, lambda spectra, parts: spectra, adjoint, returned)
    outgoing = by_source(forward_product(model, flat_kernel, inner), outer)
    imaged = exchange(outgoing, outer, 1)
    image = weights * to_traces(imaged, table)
    second = by_frequency(exchange(to_spectra(weights * image, table), outer, 2), outer)
    normal = adjoint_product(second, flat_kernel, inner)
    changed = exchange(by_source(normal, outer), outer, 3)

    double, points = returned.shape[1:]
    depth = freq_bins.shape[0] * double
    eye = jnp.eye(double, dtype=jnp.bfloat16)
    mixing = (same.astype(jnp.bfloat16)[:, None, :, None] * eye[None, :, None, :]).reshape(
        depth, depth
    )
    flat_g = returned.reshape(depth, points)
    flat_h = changed.reshape(depth, points)
    mixed_g = jnp.dot(mixing, flat_g, preferred_element_type=jnp.float32)
    mixed_h = jnp.dot(mixing, flat_h, preferred_element_type=jnp.float32)
    sums = jnp.stack(
        [
            jnp.sum(flat_g.astype(jnp.float32) * mixed_g),
            jnp.sum(image * image),
            jnp.sum(mixed_g * flat_h.astype(jnp.float32)),
            jnp.sum(flat_h.astype(jnp.float32) * mixed_h),
        ]
    )
    sums = jnp.broadcast_to(jnp.tile(sums, 2)[:, None], (8, 128))
    sums = total(total(sums, inner, "ma", 4), outer, "gx", 5)
    if recorded.shape[1] % 8 == 0:
        return tuple(
            final_step(
                sums, recorded, window_start, window_stop, returned, imaged, changed, table
            )
        )
    gradient = to_traces(returned, table)
    change = to_traces(changed, table)
    norm_start, norm_data, cross, norm_change = sums[0, 0], sums[1, 0], sums[2, 0], sums[3, 0]
    step_size = norm_start / (norm_data + epsilon)
    norm_final = norm_start - 2.0 * step_size * cross + step_size * step_size * norm_change
    solution = step_size * gradient
    residual = recorded - step_size * image
    direction = gradient - step_size * change + norm_final / (norm_start + epsilon) * gradient
    return (solution, residual, direction)


def solution(mesh):
    in_specs = (P("ma", "gx", None), P(None, "gx", "ma", None), P(), P("ma", "gx"), P("ma", "gx"))
    out_specs = (P("ma", "gx", None), P("ma", "gx", None), P("ma", "gx", None))
    return jax.shard_map(
        functools.partial(per_device, mesh.shape["gx"], mesh.shape["ma"]),
        mesh=mesh,
        in_specs=in_specs,
        out_specs=out_specs,
        check_vma=False,
    )
```
